32 devices in a mesh: vocab: 8 (over z, y), batch: 4 (over x, core).
Axes of the slice: x: 2, y: 2, z: 4, core: 2. Of those that a mesh axis runs over, the one named last changes fastest.
Arguments:
- tokens: bfloat16 [1024, 5120], P('batch'), may hold values from -180 to 180
- cluster_ids: int32 [1024, 1], P('batch'), may hold values from 0 to 3; in each aligned block of 256 rows (0 to 255, 256 to 511, ...) at most 128 rows name the same one
- head_weight: bfloat16 [5120, 4096], P('batch', 'vocab'), may hold values from -0.078125 to 0.078125
- cluster_weight: bfloat16 [5120, 4], replicated, may hold values from -0.078125 to 0.078125
- tail_proj: bfloat16 [5120, 2400], P('vocab'), may hold values from -0.078125 to 0.078125
- out_one: bfloat16 [1280, 4096], P(None, 'vocab'), may hold values from -0.15625 to 0.15625
- out_two: bfloat16 [640, 8192], P(None, 'vocab'), may hold values from -0.25 to 0.25
- out_three: bfloat16 [320, 8192], P(None, 'vocab'), may hold values from -0.3125 to 0.3125
- out_four: bfloat16 [160, 8192], P(None, 'vocab'), may hold values from -0.5 to 0.5
Outputs:
- head_logp: float32 [1024, 4096], P('batch', 'vocab')
- tail_one: float32 [512, 4096], P('batch', 'vocab')
- tail_two: float32 [512, 8192], P('batch', 'vocab')
- tail_three: float32 [512, 8192], P('batch', 'vocab')
- tail_four: float32 [512, 8192], P('batch', 'vocab')
The draws below stay inside these ranges and needn't reach their ends.
Inputs may be any that keep to these rules, and one draw needn't show every extreme that they name: `cluster_ids`: in the 256 rows of one index of batch no cluster is named by more than 128 rows.
All inputs are finite; a program needn't handle non-finite values.
Results may differ from the reference program's by a relative error of at most 0.00057.
Values may be sent and summed in bfloat16 or wider, within the bound.
No kernel may reach another device: no remote copies, remote signals or barrier semaphores. Data moves between devices by JAX's collectives and lax.ppermute only.
A program may use at most 64 MiB of HBM per device.

```python
import math
import jax
import jax.numpy as jnp
import numpy as np
from jax import lax

D = 5120
CLUSTERS = 4
P1 = 1280
P2 = 640
P3 = 320
P4 = 160
SEQ_DEV = 256
CAP = 128
SEQS = 1024
HEAD = 4096
V1 = 4096
V2 = 8192
V3 = 8192
V4 = 8192
PSUM = 2400
N_BATCH = 4


def draw_tokens(key, part):
    scale_key = jax.random.fold_in(key, 11)
    value_key = jax.random.fold_in(key, 12)
    scales = jnp.exp(jax.random.uniform(scale_key, (SEQS, 1), jnp.float32, jnp.log(3.0), jnp.log(30.0)))
    values = jnp.clip(jax.random.normal(value_key, (SEQS, D), jnp.float32), -6.0, 6.0)
    return (values * scales).astype(jnp.bfloat16)


def level_of(stream_key, dims, pieces, least, top_value):
    level, own = 1.0, jax.random.fold_in(stream_key, 6)
    for axis_at, blocks in pieces:
        draws = jnp.exp(jax.random.uniform(jax.random.fold_in(own, axis_at), (blocks,), jnp.float32, least / len(pieces), top_value / len(pieces)))
        level = level * jnp.repeat(draws, dims[axis_at] // blocks).reshape([-1 if axis == axis_at else 1 for axis in range(len(dims))])
    return level


def assign_block(key, own, number, rows, amount, top, bound, lean):
    ranking = jax.random.permutation(key, amount)
    packed, common = shares(amount, rows * top, bound, lean, True), shares(amount, rows * top, bound, lean, False)
    places = jnp.arange(amount)

    def named(tallies, rotation):
        used = int((tallies > 0).sum())
        fixed = max(1, used // 4)
        passed = fixed + (places - fixed + rotation * (used - fixed)) % max(1, amount - fixed)
        return jnp.zeros((amount,), jnp.int32).at[ranking[jnp.where(places < fixed, places, passed)]].set(jnp.asarray(tallies, jnp.int32))

    tallies = jnp.where(number % 4 == 0, named(packed, number // 4), named(common, number - number // 4 - 1))
    mixed = jax.random.permutation(jax.random.fold_in(own, 3), amount)
    giver, taker = mixed[0:amount // 2 * 2:2], mixed[1:amount // 2 * 2:2]
    slack = jnp.minimum(tallies[giver] - 1, bound - tallies[taker]) // 2
    slack = jnp.where((giver == ranking[0]) | (taker == ranking[0]) | (tallies[taker] == 0), 0, jnp.maximum(slack, 0))
    passed = jax.random.randint(jax.random.fold_in(own, 4), (amount // 2,), 0, 1 << 20) % (slack + 1)
    tallies = tallies.at[giver].add(-passed).at[taker].add(passed)
    items = jnp.searchsorted(jnp.cumsum(tallies), jnp.arange(rows * top), side="right").astype(jnp.int32)
    grid = items.reshape(top, rows).T
    grid = grid[jax.random.permutation(jax.random.fold_in(own, 1), rows)]
    rotation = jax.random.randint(jax.random.fold_in(own, 2), (rows, 1), 0, top)
    return jnp.take_along_axis(grid, (jnp.arange(top)[None, :] + rotation) % top, axis=1)


def shares(amount, total, bound, lean, full):
    loads = [(1 << 20) // math.isqrt(grade ** lean) + 1 for grade in range(1, amount + 1)]
    largest = bound if full else min(bound, max(-(-total // amount), total * loads[0] // sum(loads)))
    least = 1 if total - largest >= amount - 1 else 0
    counts, surplus = [largest] + [least] * (amount - 1), total - largest - least * (amount - 1)
    while surplus > 0:
        free = [i for i in range(1, amount) if counts[i] < largest] or [i for i in range(1, amount) if counts[i] < bound]
        mass, budget = sum([loads[i] for i in free]), surplus
        for i in free:
            extra = min(bound - counts[i], max(1, budget * loads[i] // mass), surplus)
            counts[i] = counts[i] + extra
            surplus = surplus - extra
    return np.array(counts)


def gaussian(stream_key, shape, scale, most, shards=(), kind=jnp.bfloat16):
    level = level_of(stream_key, shape, shards, -0.22, 0.18) if shards else 1.0
    values = jax.random.normal(stream_key, shape, jnp.float32) * scale * level
    return jnp.minimum(jnp.maximum(values, -most), most).astype(kind)


def setup_inputs(seed: int = 0) -> dict:
    key_list = jax.random.split(jax.random.key(seed), 10)
    tokens = draw_tokens(jax.random.fold_in(key_list[9], 71), 0)
    cluster_ids_keys = jax.random.split(jax.random.fold_in(key_list[1], 1), SEQS // SEQ_DEV)
    cluster_ids_turns = jax.random.permutation(jax.random.fold_in(key_list[1], 3), SEQS // SEQ_DEV)
    cluster_ids = jax.vmap(lambda own, number: assign_block(jax.random.fold_in(key_list[1], 2), own, number, SEQ_DEV, CLUSTERS, 1, CAP, 2))(cluster_ids_keys, cluster_ids_turns).reshape((SEQS, 1))
    head_weight = gaussian(key_list[2], (D, HEAD), D ** -0.5, 0.078125, ((0, 4), (1, 8)))
    cluster_weight = gaussian(key_list[3], (D, CLUSTERS), D ** -0.5, 0.078125)
    tail_proj = gaussian(key_list[4], (D, PSUM), D ** -0.5, 0.078125, ((0, 8),))
    out_one = gaussian(key_list[5], (P1, V1), P1 ** -0.5, 0.15625, ((1, 8),))
    out_two = gaussian(key_list[6], (P2, V2), P2 ** -0.5, 0.25, ((1, 8),))
    out_three = gaussian(key_list[7], (P3, V3), P3 ** -0.5, 0.3125, ((1, 8),))
    out_four = gaussian(key_list[8], (P4, V4), P4 ** -0.5, 0.5, ((1, 8),))
    return {"tokens": tokens, "cluster_ids": cluster_ids, "head_weight": head_weight, "cluster_weight": cluster_weight, "tail_proj": tail_proj, "out_one": out_one, "out_two": out_two, "out_three": out_three, "out_four": out_four}


def log_rows(logits):
    highest = jnp.max(logits, axis=-1, keepdims=True)
    return highest + jnp.log(jnp.sum(jnp.exp(logits - highest), axis=-1, keepdims=True))


def reference(tokens, cluster_ids, head_weight, cluster_weight, tail_proj, out_one, out_two, out_three, out_four):
    hidden = tokens.astype(jnp.float32)
    head_logits = jnp.dot(hidden, head_weight.astype(jnp.float32), precision=lax.Precision.HIGHEST)
    cluster_logits = jnp.dot(hidden, cluster_weight.astype(jnp.float32), precision=lax.Precision.HIGHEST)
    joined = jnp.concatenate([head_logits, cluster_logits], axis=1)
    log_total = log_rows(joined)
    head_logp = head_logits - log_total
    cluster_logp = cluster_logits - log_total
    cluster_of = cluster_ids[:, 0].reshape(N_BATCH, SEQ_DEV)
    labels = jnp.arange(CLUSTERS, dtype=jnp.int32)
    onehot = (cluster_of[:, :, None] == labels[None, None, :]).astype(jnp.int32)
    before = jnp.cumsum(onehot, axis=1) - onehot
    slot_of = jnp.sum(before * onehot, axis=2)
    slot_numbers = jnp.arange(CAP, dtype=jnp.int32)
    picker = ((cluster_of[:, None, None, :] == labels[None, :, None, None])
              & (slot_of[:, None, None, :] == slot_numbers[None, None, :, None])).astype(jnp.float32)
    grouped = hidden.reshape(N_BATCH, SEQ_DEV, D)
    blocks = jnp.einsum("gcjs,gsd->gcjd", picker, grouped, precision=lax.Precision.HIGHEST)
    slot_logp = jnp.einsum("gcjs,gsc->gcj", picker, cluster_logp.reshape(N_BATCH, SEQ_DEV, CLUSTERS),
                           precision=lax.Precision.HIGHEST)
    occupied = jnp.sum(picker, axis=3)
    out_weights = (out_one, out_two, out_three, out_four)
    results = []
    offset = 0
    for cluster in range(CLUSTERS):
        proj_width = out_weights[cluster].shape[0]
        block_rows = blocks[:, cluster].reshape(N_BATCH * CAP, D)
        projected = jnp.dot(block_rows, tail_proj[:, offset:offset + proj_width].astype(jnp.float32),
                            precision=lax.Precision.HIGHEST).astype(jnp.bfloat16)
        projected = lax.optimization_barrier(projected)
        offset = offset + proj_width
        logits = jnp.dot(projected.astype(jnp.float32), out_weights[cluster].astype(jnp.float32),
                         precision=lax.Precision.HIGHEST)
        scored = logits - log_rows(logits) + slot_logp[:, cluster].reshape(-1)[:, None]
        results.append(jnp.where(occupied[:, cluster].reshape(-1)[:, None] > 0, scored, jnp.zeros_like(scored)))
    return head_logp, results[0], results[1], results[2], results[3]
```

```python
import functools

import jax
import jax.numpy as jnp
from jax import lax
from jax.experimental import pallas as pl
from jax.experimental.pallas import tpu as pltpu
from jax.sharding import PartitionSpec as P

CLUSTERS = 4
CAP = 128
LANES = 128
SUBLANES = 8
F32 = jnp.float32
BF16 = jnp.bfloat16


VMEM = pl.BlockSpec(memory_space=pltpu.VMEM)
SMEM = pl.BlockSpec(memory_space=pltpu.SMEM)


def contract_rows(left, right):
    return lax.dot_general(left, right, (((0,), (0,)), ((), ())), preferred_element_type=F32)


def matmul(left, right):
    return jnp.dot(left, right, preferred_element_type=F32)


def iota(shape, axis):
    return lax.broadcasted_iota(jnp.int32, shape, axis)


def placement(ids):
    count = ids.shape[0]
    onehot = (ids == iota((count, LANES), 1)).astype(F32)
    earlier = (iota((count, count), 0) > iota((count, count), 1)).astype(BF16)
    before = matmul(earlier, onehot.astype(BF16))
    slot = jnp.sum(before * onehot, axis=1, keepdims=True)
    counts = jnp.sum(onehot, axis=0, keepdims=True)
    first, second = counts[:, 0:1], counts[:, 1:2]
    filler = before[:, 2:3] + before[:, 3:4] + first
    filler = jnp.where(filler < CAP, filler, filler + second)
    row = jnp.where(ids == 0, slot, jnp.where(ids == 1, slot + CAP, filler))
    return slot, row, counts


def row_matrix(row):
    count = row.shape[0]
    return (row.astype(jnp.int32) == iota((count, count), 1)).astype(BF16)


def partial_kernel(widths, spread, me_ref, ids_ref, columns_ref, proj_ref, *refs):
    outs, total = refs[:-1], refs[-1]
    slot, row, counts = placement(ids_ref[...])
    rows = contract_rows(row_matrix(row), columns_ref[...]).astype(BF16)
    one, two = widths[0], widths[1]
    rest = widths[2] + widths[3]
    upper, lower = rows[:CAP], rows[CAP:]
    total[:, :one] = matmul(upper, proj_ref[:, :one])
    total[:, one : one + two] = matmul(lower, proj_ref[:, one : one + two])
    others = matmul(rows, proj_ref[:, one + two :])
    number = iota((CAP, 1), 0).astype(F32)
    total[:, :rest] = jnp.where(number < counts[:, 0:1], total[:, :rest], others[:CAP])
    total[:, one : one + rest] = jnp.where(
        number < counts[:, 1:2], total[:, one : one + rest], others[CAP:]
    )
    if spread:
        chunk = outs[0].shape[0]
        for step, out in enumerate(outs):
            begin = pl.multiple_of((me_ref[0] ^ step) * chunk, chunk)
            out[...] = total[pl.ds(begin, chunk), :]
    else:
        outs[0][...] = total[...]


def sum_kernel(*refs):
    out = refs[-1]
    total = refs[0][...]
    for ref in refs[1:-1]:
        total = total + ref[...]
    out[...] = total.astype(BF16)


def unpack_kernel(ids_ref, pick_ref):
    ids = ids_ref[...]
    slot, row, counts = placement(ids)
    matrix = row_matrix(row)
    where = iota((ids.shape[0], CAP), 1)
    for at, cluster in enumerate((2, 3)):
        own = ((ids == cluster) & (slot.astype(jnp.int32) == where)).astype(BF16)
        pick_ref[at * CAP : (at + 1) * CAP, :] = contract_rows(own, matrix).astype(BF16)


def pack_columns(columns):
    lane = iota((CAP, LANES), 1)
    square = jnp.zeros((CAP, LANES), F32)
    for at, column in enumerate(columns):
        square = jnp.where(lane == at, column, square)
    return square.T[:SUBLANES]


def row_stats(values):
    top = jnp.max(values, axis=1, keepdims=True)
    return top, jnp.sum(jnp.exp(values - top), axis=1, keepdims=True)


def head_first_kernel(pieces, at_ref, tokens_ref, *refs):
    weights, out = refs[:pieces], refs[-1]
    total = None
    for step, weight in enumerate(weights):
        depth = weight.shape[0]
        begin = pl.multiple_of(at_ref[step] * depth, depth)
        part = matmul(tokens_ref[:, pl.ds(begin, depth)], weight[...])
        total = part if total is None else total + part
    out[...] = total


def head_last_kernel(pieces, at_ref, tokens_ref, *refs):
    weights, start, out, stats = refs[:pieces], refs[-3], refs[-2], refs[-1]
    total = start[...]
    for step, weight in enumerate(weights):
        depth = weight.shape[0]
        begin = pl.multiple_of(at_ref[step] * depth, depth)
        total = total + matmul(tokens_ref[:, pl.ds(begin, depth)], weight[...])
    out[...] = total
    top, mass = row_stats(total)
    stats[:SUBLANES] = pack_columns((top[:CAP], top[CAP:]))
    stats[SUBLANES:] = pack_columns((mass[:CAP], mass[CAP:]))


def score_kernel(widths, spread, me_ref, head_ref, pick_ref, one_ref, two_ref, three_ref, four_ref, *refs):
    chunks = refs[:-6]
    scores, stats, joined = refs[-6:-2], refs[-2], refs[-1]
    if spread:
        chunk = chunks[0].shape[0]
        for step, ref in enumerate(chunks):
            begin = pl.multiple_of((me_ref[0] ^ step) * chunk, chunk)
            joined[pl.ds(begin, chunk), :] = ref[...]
    else:
        joined[...] = chunks[0][...]
    one, two = widths[0], widths[1]
    rest = widths[2] + widths[3]
    small = jnp.concatenate([joined[:, :rest], joined[:, one : one + rest]], axis=0)
    picked = matmul(pick_ref[...], small).astype(BF16)
    lefts = (
        joined[:, :one],
        joined[:, one : one + two],
        picked[:CAP, : widths[2]],
        picked[CAP:, widths[2] : rest],
    )
    tops, masses = [], []
    for left, weight, score in zip(lefts, (one_ref, two_ref, three_ref, four_ref), scores):
        value = matmul(left, weight[...])
        score[...] = value
        top, mass = row_stats(value)
        tops.append(top)
        masses.append(mass)
    zero = jnp.zeros((CAP, 1), F32)
    stats[:SUBLANES] = jnp.where(
        iota((SUBLANES, CAP), 0) < 2, head_ref[:SUBLANES], pack_columns([zero, zero] + tops)
    )
    stats[SUBLANES:] = jnp.where(
        iota((SUBLANES, CAP), 0) < 2, head_ref[SUBLANES:], pack_columns([zero, zero] + masses)
    )


def merge(own, other):
    top = jnp.maximum(own[:SUBLANES], other[:SUBLANES])
    mass = own[SUBLANES:] * jnp.exp(own[:SUBLANES] - top) + other[SUBLANES:] * jnp.exp(
        other[:SUBLANES] - top
    )
    return top, mass


def merge_kernel(own_ref, other_ref, out_ref):
    top, mass = merge(own_ref[...], other_ref[...])
    out_ref[:SUBLANES] = top
    out_ref[SUBLANES:] = mass


def columns_of(rows):
    return jnp.concatenate([rows, jnp.zeros((LANES - SUBLANES, CAP), F32)], axis=0).T


def output_kernel(own_ref, other_ref, ids_ref, cluster_ref, head_ref, *refs):
    scores, head_out, outs = refs[:CLUSTERS], refs[CLUSTERS], refs[CLUSTERS + 1 :]
    top, mass = merge(own_ref[...], other_ref[...])
    tops, masses = columns_of(top), columns_of(mass)
    head_top = jnp.concatenate([tops[:, 0:1], tops[:, 1:2]], axis=0)
    head_mass = jnp.concatenate([masses[:, 0:1], masses[:, 1:2]], axis=0)
    cluster_logits = cluster_ref[...]
    overall = jnp.maximum(head_top, jnp.max(cluster_logits, axis=1, keepdims=True))
    denominator = head_mass * jnp.exp(head_top - overall) + jnp.sum(
        jnp.exp(cluster_logits - overall), axis=1, keepdims=True
    )
    log_total = overall + jnp.log(denominator)
    head_out[...] = head_ref[...] - log_total
    ids = ids_ref[...]
    slot, row, counts = placement(ids)
    own_logit = jnp.sum(
        jnp.where(ids == iota(cluster_logits.shape, 1), cluster_logits, 0.0), axis=1, keepdims=True
    )
    own_logp = own_logit - log_total
    where = iota((ids.shape[0], CAP), 1)
    here = slot.astype(jnp.int32) == where
    shifts = [
        jnp.sum(jnp.where((ids == cluster) & here, own_logp, 0.0), axis=0, keepdims=True)
        for cluster in range(CLUSTERS)
    ]
    zero = jnp.zeros((1, CAP), F32)
    shift = columns_of(jnp.concatenate(shifts + [zero] * (SUBLANES - CLUSTERS), axis=0))
    number = iota((CAP, 1), 0).astype(F32)
    for cluster in range(CLUSTERS):
        tail_log = tops[:, 2 + cluster : 3 + cluster] + jnp.log(masses[:, 2 + cluster : 3 + cluster])
        outs[cluster][...] = jnp.where(
            number < counts[:, cluster : cluster + 1],
            scores[cluster][...] - tail_log + shift[:, cluster : cluster + 1],
            0.0,
        )


def shapes(*pairs):
    return [jax.ShapeDtypeStruct(shape, kind) for shape, kind in pairs]


def cost(flops, size):
    return pl.CostEstimate(flops=int(flops), bytes_accessed=int(size), transcendentals=0)


def shards(
    sizes,
    tokens,
    cluster_ids,
    head_weight,
    cluster_weight,
    tail_proj,
    out_one,
    out_two,
    out_three,
    out_four,
):
    members, groups = sizes
    me = lax.axis_index("vocab")
    mine = lax.axis_index("batch")
    out_weights = (out_one, out_two, out_three, out_four)
    widths = tuple(weight.shape[0] for weight in out_weights)
    packed = widths[0] + widths[1]
    chunk = CAP // members
    spread = chunk % 16 == 0
    count = tokens.shape[0]

    def exchange(value, axis, size, step):
        return lax.ppermute(value, axis, [(at, at ^ step) for at in range(size)])

    features = tail_proj.shape[0]
    own_columns = lax.dynamic_slice_in_dim(tokens, me * features, features, 1)
    me_index = me.reshape(1).astype(jnp.int32)
    parts = pl.pallas_call(
        functools.partial(partial_kernel, widths, spread),
        out_shape=shapes(*([((chunk, packed), F32)] * members if spread else [((CAP, packed), F32)])),
        in_specs=[SMEM, VMEM, VMEM, VMEM],
        out_specs=[VMEM] * (members if spread else 1),
        scratch_shapes=[pltpu.VMEM((CAP, packed), F32)],
        cost_estimate=cost(2 * count * features * 2 * packed, 4 * features * packed),
        name="partial",
    )(me_index, cluster_ids, own_columns, tail_proj)
    if not spread:
        parts = [
            lax.dynamic_slice_in_dim(parts[0], (me ^ step) * chunk, chunk, 0) for step in range(members)
        ]
    arrived = [parts[0]] + [exchange(parts[step], "vocab", members, step) for step in range(1, members)]
    own = pl.pallas_call(
        sum_kernel,
        out_shape=shapes(((chunk, packed), BF16))[0],
        in_specs=[VMEM] * members,
        out_specs=VMEM,
        cost_estimate=cost(members * chunk * packed, 4 * members * chunk * packed),
        name="total",
    )(*arrived)
    chunks = [own] + [exchange(own, "vocab", members, step) for step in range(1, members)]
    if not spread:
        stacked = jnp.stack(chunks)
        order = me ^ jnp.arange(members)
        chunks = [jnp.take(stacked, order, axis=0).reshape(CAP, packed)]

    steps = [step for step in range(0, groups, 2)]
    far = [head_weight if step == 0 else exchange(head_weight, "batch", groups, step) for step in steps]
    near = [exchange(value, "batch", groups, 1) for value in far]
    at_first = jnp.stack([mine, mine ^ 1]).astype(jnp.int32)
    vocab = head_weight.shape[1]
    depth = head_weight.shape[0]
    head_start = pl.pallas_call(
        functools.partial(head_first_kernel, 2),
        out_shape=shapes(((count, vocab), F32))[0],
        in_specs=[SMEM, VMEM, VMEM, VMEM],
        out_specs=VMEM,
        cost_estimate=cost(2 * count * vocab * depth * 2, depth * vocab * 4),
        name="head_first",
    )(at_first, tokens, far[0], near[0])
    rest, at_rest = [], []
    for step, one, two in zip(steps[1:], far[1:], near[1:]):
        rest += [one, two]
        at_rest += [mine ^ step, mine ^ step ^ 1]
    head_logits, head_stats = pl.pallas_call(
        functools.partial(head_last_kernel, len(rest)),
        out_shape=shapes(((count, vocab), F32), ((2 * SUBLANES, CAP), F32)),
        in_specs=[SMEM] + [VMEM] * (len(rest) + 2),
        out_specs=[VMEM] * 2,
        cost_estimate=cost(2 * count * vocab * depth * len(rest), depth * vocab * 4),
        name="head_last",
    )(jnp.stack(at_rest).astype(jnp.int32), tokens, *rest, head_start)
    cluster_logits = matmul(tokens, cluster_weight)

    pick = pl.pallas_call(
        unpack_kernel,
        out_shape=shapes(((2 * CAP, count), BF16))[0],
        in_specs=[VMEM],
        out_specs=VMEM,
        cost_estimate=cost(2 * count * count * count * 2, 4 * count * count),
        name="unpack",
    )(cluster_ids)
    score_shapes = [((CAP, weight.shape[1]), F32) for weight in out_weights]
    *scores, stats = pl.pallas_call(
        functools.partial(score_kernel, widths, spread),
        out_shape=shapes(*score_shapes, ((2 * SUBLANES, CAP), F32)),
        in_specs=[SMEM] + [VMEM] * (6 + len(chunks)),
        out_specs=[VMEM] * (CLUSTERS + 1),
        scratch_shapes=[pltpu.VMEM((CAP, packed), BF16)],
        cost_estimate=cost(
            2 * CAP * sum(weight.size for weight in out_weights), 2 * sum(weight.size for weight in out_weights)
        ),
        name="scores",
    )(me_index, head_stats, pick, *out_weights, *chunks)

    step = 1
    while 2 * step < members:
        stats = pl.pallas_call(
            merge_kernel,
            out_shape=shapes(((2 * SUBLANES, CAP), F32))[0],
            in_specs=[VMEM] * 2,
            out_specs=VMEM,
            cost_estimate=cost(8 * CAP * SUBLANES, 24 * CAP * SUBLANES),
            name="merge",
        )(stats, exchange(stats, "vocab", members, step))
        step = 2 * step
    other = exchange(stats, "vocab", members, step)
    out_shapes = [((count, vocab), F32)] + score_shapes
    return tuple(
        pl.pallas_call(
            output_kernel,
            out_shape=shapes(*out_shapes),
            in_specs=[VMEM] * (5 + CLUSTERS),
            out_specs=[VMEM] * (1 + CLUSTERS),
            cost_estimate=cost(count * vocab * 8, 8 * count * vocab * 8),
            name="outputs",
        )(stats, other, cluster_ids, cluster_logits, head_logits, *scores)
    )


def solution(mesh):
    in_specs = (
        P("batch", None),
        P("batch", None),
        P("batch", "vocab"),
        P(),
        P("vocab", None),
        P(None, "vocab"),
        P(None, "vocab"),
        P(None, "vocab"),
        P(None, "vocab"),
    )
    out_specs = (P("batch", "vocab"),) * 5
    sizes = (mesh.shape["vocab"], mesh.shape["batch"])
    return jax.shard_map(
        functools.partial(shards, sizes), mesh=mesh, in_specs=in_specs, out_specs=out_specs, check_vma=False
    )
```

```python
import functools

import jax
import jax.numpy as jnp
from jax import lax
from jax.experimental import pallas as pl
from jax.experimental.pallas import tpu as pltpu
from jax.sharding import PartitionSpec as P

CLUSTERS = 4
CAP = 128
LANES = 128
SUBLANES = 8
F32 = jnp.float32
BF16 = jnp.bfloat16


VMEM = pl.BlockSpec(memory_space=pltpu.VMEM)
SMEM = pl.BlockSpec(memory_space=pltpu.SMEM)
HBM = pl.BlockSpec(memory_space=pltpu.HBM)


def contract_rows(left, right):
    return lax.dot_general(left, right, (((0,), (0,)), ((), ())), preferred_element_type=F32)


def matmul(left, right):
    return jnp.dot(left, right, preferred_element_type=F32)


def iota(shape, axis):
    return lax.broadcasted_iota(jnp.int32, shape, axis)


def placement(ids):
    count = ids.shape[1]
    onehot = (ids == iota((SUBLANES, count), 0)).astype(F32)
    earlier = (iota((count, count), 0) < iota((count, count), 1)).astype(BF16)
    before = matmul(onehot.astype(BF16), earlier)
    slot = jnp.sum(before * onehot, axis=0, keepdims=True)
    counts = jnp.sum(onehot, axis=1, keepdims=True)
    first, second = counts[0:1], counts[1:2]
    filler = before[2:3] + before[3:4] + first
    filler = jnp.where(filler < CAP, filler, filler + second)
    row = jnp.where(ids == 0, slot, jnp.where(ids == 1, slot + CAP, filler))
    return slot.astype(jnp.int32), row.astype(jnp.int32), counts


def row_matrix(row):
    count = row.shape[1]
    return (row == iota((count, count), 0)).astype(BF16)


def contract_last(left, right):
    return lax.dot_general(left, right, (((1,), (1,)), ((), ())), preferred_element_type=F32)


def partial_kernel(widths, spread, me_ref, ids_ref, columns_ref, proj_ref, *refs):
    outs, columns, proj, total, sems = refs[:-4], refs[-4], refs[-3], refs[-2], refs[-1]
    one, two = widths[0], widths[1]
    rest = widths[2] + widths[3]
    features = columns.shape[1]
    if columns_ref.shape[1] == features:
        source = columns_ref
    else:
        source = columns_ref.at[:, pl.ds(pl.multiple_of(me_ref[0] * features, LANES), features)]
    ranges = ((one + two, rest), (0, one), (one, two))
    copies = [pltpu.make_async_copy(source, columns, sems.at[0])]
    for at, (begin, size) in enumerate(ranges):
        copies.append(
            pltpu.make_async_copy(
                proj_ref.at[pl.ds(begin, size), :], proj.at[pl.ds(begin, size), :], sems.at[1 + at]
            )
        )
    for copy in copies:
        copy.start()
    slot, row, counts = placement(ids_ref[...])
    matrix = row_matrix(row)
    copies[0].wait()
    rows = matmul(matrix, columns[...]).astype(BF16)
    upper, lower = rows[:CAP], rows[CAP:]
    number = iota((CAP, 1), 0).astype(F32)
    copies[1].wait()
    others = contract_last(rows, proj[one + two :])
    copies[2].wait()
    whole = contract_last(upper, proj[:one])
    total[:, rest:one] = whole[:, rest:]
    total[:, :rest] = jnp.where(number < counts[0:1], whole[:, :rest], others[:CAP])
    copies[3].wait()
    whole = contract_last(lower, proj[one : one + two])
    total[:, one + rest :] = whole[:, rest:]
    total[:, one : one + rest] = jnp.where(number < counts[1:2], whole[:, :rest], others[CAP:])
    if spread:
        chunk = outs[0].shape[0]
        for step, out in enumerate(outs):
            begin = pl.multiple_of((me_ref[0] ^ step) * chunk, chunk)
            out[...] = total[pl.ds(begin, chunk), :]
    else:
        outs[0][...] = total[...]


def unpack_kernel(ids_ref, pick_ref):
    ids = ids_ref[...]
    slot, row, counts = placement(ids)
    matrix = row_matrix(row)
    where = iota((CAP, ids.shape[1]), 0)
    for at, cluster in enumerate((2, 3)):
        own = ((ids == cluster) & (slot == where)).astype(BF16)
        pick_ref[at * CAP : (at + 1) * CAP, :] = contract_last(own, matrix).astype(BF16)


def pack_columns(columns):
    lane = iota((CAP, LANES), 1)
    square = jnp.zeros((CAP, LANES), F32)
    for at, column in enumerate(columns):
        square = jnp.where(lane == at, column, square)
    return square.T[:SUBLANES]


def row_stats(values):
    top = jnp.max(values, axis=1, keepdims=True)
    return top, jnp.sum(jnp.exp(values - top), axis=1, keepdims=True)


def head_first_kernel(pieces, at_ref, tokens_ref, *refs):
    weights, out = refs[:pieces], refs[-1]
    total = None
    for step, weight in enumerate(weights):
        depth = weight.shape[0]
        begin = pl.multiple_of(at_ref[step] * depth, depth)
        part = matmul(tokens_ref[:, pl.ds(begin, depth)], weight[...])
        total = part if total is None else total + part
    out[...] = total


def head_last_kernel(pieces, at_ref, tokens_ref, *refs):
    weights, start, out, stats = refs[:pieces], refs[-3], refs[-2], refs[-1]
    total = start[...]
    for step, weight in enumerate(weights):
        depth = weight.shape[0]
        begin = pl.multiple_of(at_ref[step] * depth, depth)
        total = total + matmul(tokens_ref[:, pl.ds(begin, depth)], weight[...])
    out[...] = total
    top, mass = row_stats(total)
    stats[:SUBLANES] = pack_columns((top[:CAP], top[CAP:]))
    stats[SUBLANES:] = pack_columns((mass[:CAP], mass[CAP:]))


def score_kernel(widths, spread, me_ref, head_ref, pick_ref, one_ref, two_ref, three_ref, four_ref, *refs):
    chunks = refs[:-6]
    scores, stats, joined = refs[-6:-2], refs[-2], refs[-1]
    if spread:
        chunk = chunks[0].shape[0]
        for step, ref in enumerate(chunks):
            begin = pl.multiple_of((me_ref[0] ^ step) * chunk, chunk)
            joined[pl.ds(begin, chunk), :] = ref[...]
    else:
        joined[...] = chunks[0][...]
    one, two = widths[0], widths[1]
    rest = widths[2] + widths[3]
    small = jnp.concatenate([joined[:, :rest], joined[:, one : one + rest]], axis=0)
    picked = matmul(pick_ref[...], small).astype(BF16)
    lefts = (
        joined[:, :one],
        joined[:, one : one + two],
        picked[:CAP, : widths[2]],
        picked[CAP:, widths[2] : rest],
    )
    tops, masses = [], []
    for left, weight, score in zip(lefts, (one_ref, two_ref, three_ref, four_ref), scores):
        value = matmul(left, weight[...])
        score[...] = value
        top, mass = row_stats(value)
        tops.append(top)
        masses.append(mass)
    zero = jnp.zeros((CAP, 1), F32)
    stats[:SUBLANES] = jnp.where(
        iota((SUBLANES, CAP), 0) < 2, head_ref[:SUBLANES], pack_columns([zero, zero] + tops)
    )
    stats[SUBLANES:] = jnp.where(
        iota((SUBLANES, CAP), 0) < 2, head_ref[SUBLANES:], pack_columns([zero, zero] + masses)
    )


def merge(own, other):
    top = jnp.maximum(own[:SUBLANES], other[:SUBLANES])
    mass = own[SUBLANES:] * jnp.exp(own[:SUBLANES] - top) + other[SUBLANES:] * jnp.exp(
        other[:SUBLANES] - top
    )
    return top, mass


def columns_of(rows):
    return jnp.concatenate([rows, jnp.zeros((LANES - SUBLANES, CAP), F32)], axis=0).T


def output_kernel(own_ref, other_ref, ids_ref, cluster_ref, head_ref, *refs):
    scores, head_out, outs = refs[:CLUSTERS], refs[CLUSTERS], refs[CLUSTERS + 1 :]
    ids = ids_ref[...]
    slot, row, counts = placement(ids)
    cluster_logits = cluster_ref[...]
    own_logit = jnp.sum(
        jnp.where(ids == iota(cluster_logits.shape, 0), cluster_logits, 0.0), axis=0, keepdims=True
    )
    top, mass = merge(own_ref[...], other_ref[...])
    head_top = jnp.concatenate([top[0:1], top[1:2]], axis=1)
    head_mass = jnp.concatenate([mass[0:1], mass[1:2]], axis=1)
    overall = jnp.maximum(head_top, jnp.max(cluster_logits, axis=0, keepdims=True))
    denominator = head_mass * jnp.exp(head_top - overall) + jnp.sum(
        jnp.exp(cluster_logits - overall), axis=0, keepdims=True
    )
    log_total = overall + jnp.log(denominator)
    number = iota((SUBLANES, CAP), 0)
    logs = jnp.where(
        number == 0, log_total[:, :CAP], jnp.where(number == 1, log_total[:, CAP:], top + jnp.log(mass))
    )
    columns = columns_of(logs)
    head_out[:CAP] = head_ref[:CAP] - columns[:, 0:1]
    head_out[CAP:] = head_ref[CAP:] - columns[:, 1:2]
    own_logp = own_logit - log_total
    here = slot == iota((CAP, ids.shape[1]), 0)
    number = iota((CAP, 1), 0).astype(F32)
    for cluster in range(CLUSTERS):
        slot_logp = jnp.sum(jnp.where((ids == cluster) & here, own_logp, 0.0), axis=1, keepdims=True)
        shift = columns[:, 2 + cluster : 3 + cluster] - slot_logp
        outs[cluster][...] = jnp.where(
            number < counts[cluster : cluster + 1], scores[cluster][...] - shift, 0.0
        )


def shapes(*pairs):
    return [jax.ShapeDtypeStruct(shape, kind) for shape, kind in pairs]


def limit(mebibytes):
    return pltpu.CompilerParams(vmem_limit_bytes=mebibytes * 2**20)


def cost(flops, size):
    return pl.CostEstimate(flops=int(flops), bytes_accessed=int(size), transcendentals=0)


def shards(
    sizes,
    tokens,
    cluster_ids,
    head_weight,
    cluster_weight,
    tail_proj,
    out_one,
    out_two,
    out_three,
    out_four,
):
    members, groups = sizes
    me = lax.axis_index("vocab")
    mine = lax.axis_index("batch")
    out_weights = (out_one, out_two, out_three, out_four)
    widths = tuple(weight.shape[0] for weight in out_weights)
    packed = widths[0] + widths[1]
    chunk = CAP // members
    spread = chunk % 16 == 0
    count = tokens.shape[0]

    def exchange(value, axis, size, step):
        return lax.ppermute(value, axis, [(at, at ^ step) for at in range(size)])

    features = tail_proj.shape[0]
    ids = cluster_ids.T
    if features % LANES:
        columns = lax.dynamic_slice_in_dim(tokens, me * features, features, 1)
    else:
        columns = tokens
    me_index = me.reshape(1).astype(jnp.int32)
    parts = pl.pallas_call(
        functools.partial(partial_kernel, widths, spread),
        out_shape=shapes(*([((chunk, packed), F32)] * members if spread else [((CAP, packed), F32)])),
        in_specs=[SMEM, VMEM, HBM, HBM],
        out_specs=[VMEM] * (members if spread else 1),
        scratch_shapes=[
            pltpu.VMEM((count, features), BF16),
            pltpu.VMEM(tail_proj.shape[::-1], BF16),
            pltpu.VMEM((CAP, packed), F32),
            pltpu.SemaphoreType.DMA((4,)),
        ],
        compiler_params=limit(16),
        cost_estimate=cost(2 * count * features * 2 * packed, 4 * features * packed),
        name="partial",
    )(me_index, ids, columns, tail_proj.T)
    if not spread:
        parts = [
            lax.dynamic_slice_in_dim(parts[0], (me ^ step) * chunk, chunk, 0) for step in range(members)
        ]
    arrived = [parts[0]] + [exchange(parts[step], "vocab", members, step) for step in range(1, members)]

    steps = [step for step in range(0, groups, 2)]
    far = [exchange(head_weight, "batch", groups, step) for step in steps[1:]]
    near = exchange(head_weight, "batch", groups, 1)
    at_first = jnp.stack([mine, mine ^ 1]).astype(jnp.int32)
    vocab = head_weight.shape[1]
    depth = head_weight.shape[0]
    head_start = pl.pallas_call(
        functools.partial(head_first_kernel, 2),
        out_shape=shapes(((count, vocab), F32))[0],
        in_specs=[SMEM, VMEM, VMEM, VMEM],
        out_specs=VMEM,
        compiler_params=limit(12),
        cost_estimate=cost(2 * count * vocab * depth * 2, depth * vocab * 4),
        name="head_first",
    )(at_first, tokens, head_weight, near)
    pick = pl.pallas_call(
        unpack_kernel,
        out_shape=shapes(((2 * CAP, count), BF16))[0],
        in_specs=[VMEM],
        out_specs=VMEM,
        compiler_params=limit(8),
        cost_estimate=cost(2 * count * count * count * 2, 4 * count * count),
        name="unpack",
    )(ids)
    cluster_logits = lax.dot_general(
        cluster_weight, tokens, (((0,), (1,)), ((), ())), preferred_element_type=F32
    )
    arrived, head_start, pick, cluster_logits = lax.optimization_barrier(
        (arrived, head_start, pick, cluster_logits)
    )
    own = sum(arrived[1:], arrived[0]).astype(BF16)
    own, far = lax.optimization_barrier((own, far))
    chunks = [own] + [exchange(own, "vocab", members, step) for step in range(1, members)]
    if not spread:
        stacked = jnp.stack(chunks)
        order = me ^ jnp.arange(members)
        chunks = [jnp.take(stacked, order, axis=0).reshape(CAP, packed)]

    rest, at_rest = [], []
    for step, value in zip(steps[1:], far):
        rest += [value, exchange(value, "batch", groups, 1)]
        at_rest += [mine ^ step, mine ^ step ^ 1]
    head_logits, head_stats = pl.pallas_call(
        functools.partial(head_last_kernel, len(rest)),
        out_shape=shapes(((count, vocab), F32), ((2 * SUBLANES, CAP), F32)),
        in_specs=[SMEM] + [VMEM] * (len(rest) + 2),
        out_specs=[VMEM] * 2,
        compiler_params=limit(12),
        cost_estimate=cost(2 * count * vocab * depth * len(rest), depth * vocab * 4),
        name="head_last",
    )(jnp.stack(at_rest).astype(jnp.int32), tokens, *rest, head_start)
    score_shapes = [((CAP, weight.shape[1]), F32) for weight in out_weights]
    *scores, stats = pl.pallas_call(
        functools.partial(score_kernel, widths, spread),
        out_shape=shapes(*score_shapes, ((2 * SUBLANES, CAP), F32)),
        in_specs=[SMEM] + [VMEM] * (6 + len(chunks)),
        out_specs=[VMEM] * (CLUSTERS + 1),
        scratch_shapes=[pltpu.VMEM((CAP, packed), BF16)],
        compiler_params=limit(16),
        cost_estimate=cost(
            2 * CAP * sum(weight.size for weight in out_weights), 2 * sum(weight.size for weight in out_weights)
        ),
        name="scores",
    )(me_index, head_stats, pick, *out_weights, *chunks)

    step = 1
    while 2 * step < members:
        stats = jnp.concatenate(merge(stats, exchange(stats, "vocab", members, step)), axis=0)
        step = 2 * step
    other = exchange(stats, "vocab", members, step)
    out_shapes = [((count, vocab), F32)] + score_shapes
    return tuple(
        pl.pallas_call(
            output_kernel,
            out_shape=shapes(*out_shapes),
            in_specs=[VMEM] * (5 + CLUSTERS),
            out_specs=[VMEM] * (1 + CLUSTERS),
            compiler_params=limit(12),
        cost_estimate=cost(count * vocab * 8, 8 * count * vocab * 8),
            name="outputs",
        )(stats, other, ids, cluster_logits, head_logits, *scores)
    )


def solution(mesh):
    in_specs = (
        P("batch", None),
        P("batch", None),
        P("batch", "vocab"),
        P(),
        P("vocab", None),
        P(None, "vocab"),
        P(None, "vocab"),
        P(None, "vocab"),
        P(None, "vocab"),
    )
    out_specs = (P("batch", "vocab"),) * 5
    sizes = (mesh.shape["vocab"], mesh.shape["batch"])
    return jax.shard_map(
        functools.partial(shards, sizes), mesh=mesh, in_specs=in_specs, out_specs=out_specs, check_vma=False
    )
```

```python
import functools

import jax
import jax.numpy as jnp
from jax import lax
from jax.experimental import pallas as pl
from jax.experimental.pallas import tpu as pltpu
from jax.sharding import PartitionSpec as P


CLUSTERS = 4
CAP = 128
LANES = 128
SUBLANES = 8
F32 = jnp.float32
BF16 = jnp.bfloat16


VMEM = pl.BlockSpec(memory_space=pltpu.VMEM)
SMEM = pl.BlockSpec(memory_space=pltpu.SMEM)
HBM = pl.BlockSpec(memory_space=pltpu.HBM)


def matmul(left, right):
    return jnp.dot(left, right, preferred_element_type=F32)


def iota(shape, axis):
    return lax.broadcasted_iota(jnp.int32, shape, axis)


def placement(ids):
    count = ids.shape[1]
    onehot = (ids == iota((SUBLANES, count), 0)).astype(F32)
    earlier = (iota((count, count), 0) < iota((count, count), 1)).astype(BF16)
    before = matmul(onehot.astype(BF16), earlier)
    slot = jnp.sum(before * onehot, axis=0, keepdims=True)
    counts = jnp.sum(onehot, axis=1, keepdims=True)
    first, second = counts[0:1], counts[1:2]
    filler = before[2:3] + before[3:4] + first
    filler = jnp.where(filler < CAP, filler, filler + second)
    row = jnp.where(ids == 0, slot, jnp.where(ids == 1, slot + CAP, filler))
    return slot.astype(jnp.int32), row.astype(jnp.int32), counts


def row_matrix(row):
    count = row.shape[1]
    return (row == iota((count, count), 0)).astype(BF16)


def contract_last(left, right):
    return lax.dot_general(left, right, (((1,), (1,)), ((), ())), preferred_element_type=F32)


def partial_kernel(widths, spread, me_ref, ids_ref, columns_ref, proj_ref, *refs):
    outs, (ids, columns, proj, total, sems) = refs[:-5], refs[-5:]
    one, two = widths[0], widths[1]
    rest = widths[2] + widths[3]
    features = columns.shape[1]
    if columns_ref.shape[1] == features:
        source = columns_ref
    else:
        source = columns_ref.at[:, pl.ds(pl.multiple_of(me_ref[0] * features, LANES), features)]
    ranges = ((one + two, rest), (0, one), (one, two))
    copies = [pltpu.make_async_copy(source, columns, sems.at[0])]
    first_copy = pltpu.make_async_copy(ids_ref, ids, sems.at[4])
    first_copy.start()
    for at, (begin, size) in enumerate(ranges):
        copies.append(
            pltpu.make_async_copy(
                proj_ref.at[pl.ds(begin, size), :], proj.at[pl.ds(begin, size), :], sems.at[1 + at]
            )
        )
    for copy in copies:
        copy.start()
    first_copy.wait()
    _, row, counts = placement(ids[...])
    matrix = row_matrix(row)
    copies[0].wait()
    rows = matmul(matrix, columns[...]).astype(BF16)
    upper, lower = rows[:CAP], rows[CAP:]
    number = iota((CAP, 1), 0).astype(F32)
    copies[1].wait()
    others = contract_last(rows, proj[one + two :])
    copies[2].wait()
    whole = contract_last(upper, proj[:one])
    total[:, rest:one] = whole[:, rest:]
    total[:, :rest] = jnp.where(number < counts[0:1], whole[:, :rest], others[:CAP])
    copies[3].wait()
    whole = contract_last(lower, proj[one : one + two])
    total[:, one + rest :] = whole[:, rest:]
    total[:, one : one + rest] = jnp.where(number < counts[1:2], whole[:, :rest], others[CAP:])
    if spread:
        chunk = outs[0].shape[0]
        for step, out in enumerate(outs):
            begin = pl.multiple_of((me_ref[0] ^ step) * chunk, chunk)
            out[...] = total[pl.ds(begin, chunk), :]
    else:
        outs[0][...] = total[...]


def unpack_kernel(ids_ref, pick_ref):
    ids = ids_ref[...]
    slot, row, _ = placement(ids)
    matrix = row_matrix(row)
    where = iota((CAP, ids.shape[1]), 0)
    for at, cluster in enumerate((2, 3)):
        own = ((ids == cluster) & (slot == where)).astype(BF16)
        pick_ref[at * CAP : (at + 1) * CAP, :] = contract_last(own, matrix).astype(BF16)


def pack_columns(columns):
    lane = iota((CAP, LANES), 1)
    square = jnp.zeros((CAP, LANES), F32)
    for at, column in enumerate(columns):
        square = jnp.where(lane == at, column, square)
    return square.T[:SUBLANES]


def row_stats(values):
    top = jnp.max(values, axis=1, keepdims=True)
    return top, jnp.sum(jnp.exp(values - top), axis=1, keepdims=True)


def head_more_kernel(steps, mine_ref, tokens_ref, *refs):
    weights, start, out = refs[:-2], refs[-2], refs[-1]
    total = start[...]
    for step, weight in zip(steps, weights):
        depth = weight.shape[0]
        begin = pl.multiple_of((mine_ref[0] ^ step) * depth, depth)
        total = total + matmul(tokens_ref[:, pl.ds(begin, depth)], weight[...])
    out[...] = total


def head_first_kernel(steps, mine_ref, tokens_ref, *refs):
    weights, out = refs[:-1], refs[-1]
    total = None
    for step, weight in zip(steps, weights):
        depth = weight.shape[0]
        begin = pl.multiple_of((mine_ref[0] ^ step) * depth, depth)
        part = matmul(tokens_ref[:, pl.ds(begin, depth)], weight[...])
        total = part if total is None else total + part
    out[...] = total


def head_last_kernel(steps, mine_ref, tokens_ref, *refs):
    weights, start, out, stats = refs[:-3], refs[-3], refs[-2], refs[-1]
    total = start[...]
    for step, weight in zip(steps, weights):
        depth = weight.shape[0]
        begin = pl.multiple_of((mine_ref[0] ^ step) * depth, depth)
        total = total + matmul(tokens_ref[:, pl.ds(begin, depth)], weight[...])
    out[...] = total
    top, mass = row_stats(total)
    stats[:SUBLANES] = pack_columns((top[:CAP], top[CAP:]))
    stats[SUBLANES:] = pack_columns((mass[:CAP], mass[CAP:]))


def score_kernel(widths, spread, me_ref, pick_ref, one_ref, two_ref, three_ref, four_ref, *refs):
    chunks = refs[:-6]
    scores, stats, joined = refs[-6:-2], refs[-2], refs[-1]
    if spread:
        chunk = chunks[0].shape[0]
        for step, ref in enumerate(chunks):
            begin = pl.multiple_of((me_ref[0] ^ step) * chunk, chunk)
            joined[pl.ds(begin, chunk), :] = ref[...]
    else:
        joined[...] = chunks[0][...]
    one, two = widths[0], widths[1]
    rest = widths[2] + widths[3]
    small = jnp.concatenate([joined[:, :rest], joined[:, one : one + rest]], axis=0)
    picked = matmul(pick_ref[...], small).astype(BF16)
    lefts = (
        joined[:, :one],
        joined[:, one : one + two],
        picked[:CAP, : widths[2]],
        picked[CAP:, widths[2] : rest],
    )
    tops, masses = [], []
    for left, weight, score in zip(lefts, (one_ref, two_ref, three_ref, four_ref), scores):
        value = matmul(left, weight[...])
        score[...] = value
        top, mass = row_stats(value)
        tops.append(top)
        masses.append(mass)
    zero = jnp.zeros((CAP, 1), F32)
    stats[:SUBLANES] = pack_columns([zero, zero] + tops)
    stats[SUBLANES:] = pack_columns([zero, zero] + masses)


def merge(own, other):
    top = jnp.maximum(own[:SUBLANES], other[:SUBLANES])
    mass = own[SUBLANES:] * jnp.exp(own[:SUBLANES] - top) + other[SUBLANES:] * jnp.exp(
        other[:SUBLANES] - top
    )
    return top, mass


def columns_of(rows):
    return jnp.concatenate([rows, jnp.zeros((LANES - SUBLANES, CAP), F32)], axis=0).T


def output_kernel(own_ref, other_ref, ids_ref, cluster_ref, head_ref, *refs):
    scores, head_out, outs = refs[:CLUSTERS], refs[CLUSTERS], refs[CLUSTERS + 1 :]
    ids = ids_ref[...]
    slot, _, counts = placement(ids)
    cluster_logits = cluster_ref[...]
    own_logit = jnp.sum(
        jnp.where(ids == iota(cluster_logits.shape, 0), cluster_logits, 0.0), axis=0, keepdims=True
    )
    top, mass = merge(own_ref[...], other_ref[...])
    head_top = jnp.concatenate([top[0:1], top[1:2]], axis=1)
    head_mass = jnp.concatenate([mass[0:1], mass[1:2]], axis=1)
    overall = jnp.maximum(head_top, jnp.max(cluster_logits, axis=0, keepdims=True))
    denominator = head_mass * jnp.exp(head_top - overall) + jnp.sum(
        jnp.exp(cluster_logits - overall), axis=0, keepdims=True
    )
    log_total = overall + jnp.log(denominator)
    number = iota((SUBLANES, CAP), 0)
    logs = jnp.where(
        number == 0, log_total[:, :CAP], jnp.where(number == 1, log_total[:, CAP:], top + jnp.log(mass))
    )
    columns = columns_of(logs)
    head_out[:CAP] = head_ref[:CAP] - columns[:, 0:1]
    head_out[CAP:] = head_ref[CAP:] - columns[:, 1:2]
    own_logp = own_logit - log_total
    here = slot == iota((CAP, ids.shape[1]), 0)
    number = iota((CAP, 1), 0).astype(F32)
    for cluster in range(CLUSTERS):
        slot_logp = jnp.sum(jnp.where((ids == cluster) & here, own_logp, 0.0), axis=1, keepdims=True)
        shift = columns[:, 2 + cluster : 3 + cluster] - slot_logp
        outs[cluster][...] = jnp.where(
            number < counts[cluster : cluster + 1], scores[cluster][...] - shift, 0.0
        )


def shapes(*pairs):
    return [jax.ShapeDtypeStruct(shape, kind) for shape, kind in pairs]


def in_hbm(value):
    return pltpu.with_memory_space_constraint(value, pltpu.HBM)


def limit(mebibytes):
    return pltpu.CompilerParams(vmem_limit_bytes=mebibytes * 2**20)


def cost(flops, size):
    return pl.CostEstimate(flops=int(flops), bytes_accessed=int(size), transcendentals=0)


def shards(
    sizes,
    tokens,
    cluster_ids,
    head_weight,
    cluster_weight,
    tail_proj,
    out_one,
    out_two,
    out_three,
    out_four,
):
    members, groups = sizes
    me = lax.axis_index("vocab")
    mine = lax.axis_index("batch")
    out_weights = (out_one, out_two, out_three, out_four)
    widths = tuple(weight.shape[0] for weight in out_weights)
    packed = widths[0] + widths[1]
    chunk = CAP // members
    spread = chunk % 16 == 0
    count = tokens.shape[0]

    def exchange(value, axis, size, step):
        return lax.ppermute(value, axis, [(at, at ^ step) for at in range(size)])

    features = tail_proj.shape[0]
    ids = cluster_ids.T
    if features % LANES:
        columns = lax.dynamic_slice_in_dim(tokens, me * features, features, 1)
    else:
        columns = tokens
    me_index = me.reshape(1).astype(jnp.int32)
    parts = pl.pallas_call(
        functools.partial(partial_kernel, widths, spread),
        out_shape=shapes(*([((chunk, packed), F32)] * members if spread else [((CAP, packed), F32)])),
        in_specs=[SMEM, HBM, HBM, HBM],
        out_specs=[VMEM] * (members if spread else 1),
        scratch_shapes=[
            pltpu.VMEM((1, count), jnp.int32),
            pltpu.VMEM((count, features), BF16),
            pltpu.VMEM(tail_proj.shape[::-1], BF16),
            pltpu.VMEM((CAP, packed), F32),
            pltpu.SemaphoreType.DMA((5,)),
        ],
        compiler_params=limit(8),
        cost_estimate=cost(2 * count * features * 2 * packed, 4 * features * packed),
        name="partial",
    )(me_index, in_hbm(ids), in_hbm(columns), in_hbm(tail_proj.T))
    if not spread:
        parts = [
            lax.dynamic_slice_in_dim(parts[0], (me ^ step) * chunk, chunk, 0) for step in range(members)
        ]
    parts, head_weight = lax.optimization_barrier((parts, head_weight))
    pairs = [
        parts[step] + exchange(parts[step + 1], "vocab", members, 1)
        for step in reversed(range(0, members, 2))
    ][::-1]
    arrived = [pairs[0]] + [exchange(pairs[at], "vocab", members, 2 * at) for at in reversed(range(1, members // 2))]

    steps = [step for step in range(0, groups, 2)]
    far = [exchange(head_weight, "batch", groups, step) for step in steps[1:]]
    near = exchange(head_weight, "batch", groups, 1)
    mine_index = mine.reshape(1).astype(jnp.int32)
    vocab = head_weight.shape[1]
    depth = head_weight.shape[0]
    head_start = pl.pallas_call(
        functools.partial(head_first_kernel, (0, 1)),
        out_shape=shapes(((count, vocab), F32))[0],
        in_specs=[SMEM, VMEM, VMEM, VMEM],
        out_specs=VMEM,
        compiler_params=limit(6),
        cost_estimate=cost(2 * count * vocab * depth * 2, depth * vocab * 4),
        name="head_first",
    )(mine_index, tokens, head_weight, near)
    pick = pl.pallas_call(
        unpack_kernel,
        out_shape=shapes(((2 * CAP, count), BF16))[0],
        in_specs=[VMEM],
        out_specs=VMEM,
        compiler_params=limit(2),
        cost_estimate=cost(2 * count * count * count * 2, 4 * count * count),
        name="unpack",
    )(ids)
    cluster_logits = lax.dot_general(
        cluster_weight, tokens, (((0,), (1,)), ((), ())), preferred_element_type=F32
    )
    arrived, head_start, cluster_logits = lax.optimization_barrier((arrived, head_start, cluster_logits))
    own = sum(arrived[1:], arrived[0]).astype(BF16)
    evens = [own] + [exchange(own, "vocab", members, step) for step in range(2, members, 2)]
    _, far = lax.optimization_barrier((evens[-1], far))
    chunks = []
    for value in evens:
        chunks += [value, exchange(value, "vocab", members, 1)]
    if not spread:
        stacked = jnp.stack(chunks)
        order = me ^ jnp.arange(members)
        chunks = [jnp.take(stacked, order, axis=0).reshape(CAP, packed)]

    rest = [exchange(value, "batch", groups, 1) for value in far]
    head_more = pl.pallas_call(
        functools.partial(head_more_kernel, tuple(steps[1:])),
        out_shape=shapes(((count, vocab), F32))[0],
        in_specs=[SMEM] + [VMEM] * (len(far) + 2),
        out_specs=VMEM,
        compiler_params=limit(6),
        cost_estimate=cost(2 * count * vocab * depth * len(far), depth * vocab * 4),
        name="head_more",
    )(mine_index, tokens, *far, head_start)
    head_logits, head_stats = pl.pallas_call(
        functools.partial(head_last_kernel, tuple(step ^ 1 for step in steps[1:])),
        out_shape=shapes(((count, vocab), F32), ((2 * SUBLANES, CAP), F32)),
        in_specs=[SMEM] + [VMEM] * (len(rest) + 2),
        out_specs=[VMEM] * 2,
        compiler_params=limit(6),
        cost_estimate=cost(2 * count * vocab * depth * len(rest), depth * vocab * 4),
        name="head_last",
    )(mine_index, tokens, *rest, head_more)
    score_shapes = [((CAP, weight.shape[1]), F32) for weight in out_weights]
    *scores, stats = pl.pallas_call(
        functools.partial(score_kernel, widths, spread),
        out_shape=shapes(*score_shapes, ((2 * SUBLANES, CAP), F32)),
        in_specs=[SMEM] + [VMEM] * (5 + len(chunks)),
        out_specs=[VMEM] * (CLUSTERS + 1),
        scratch_shapes=[pltpu.VMEM((CAP, packed), BF16)],
        compiler_params=limit(6),
        cost_estimate=cost(
            2 * CAP * sum(weight.size for weight in out_weights), 2 * sum(weight.size for weight in out_weights)
        ),
        name="scores",
    )(me_index, pick, *out_weights, *chunks)

    stats = jnp.where(lax.rem(iota(stats.shape, 0), SUBLANES) < 2, head_stats, stats)
    step = 1
    while 2 * step < members:
        stats = jnp.concatenate(merge(stats, exchange(stats, "vocab", members, step)), axis=0)
        step = 2 * step
    other = exchange(stats, "vocab", members, step)
    out_shapes = [((count, vocab), F32)] + score_shapes
    return tuple(
        pl.pallas_call(
            output_kernel,
            out_shape=shapes(*out_shapes),
            in_specs=[VMEM] * (5 + CLUSTERS),
            out_specs=[VMEM] * (1 + CLUSTERS),
            compiler_params=limit(6),
        cost_estimate=cost(count * vocab * 8, 8 * count * vocab * 8),
            name="outputs",
        )(stats, other, ids, cluster_logits, head_logits, *scores)
    )


def solution(mesh):
    in_specs = (
        P("batch", None),
        P("batch", None),
        P("batch", "vocab"),
        P(),
        P("vocab", None),
        P(None, "vocab"),
        P(None, "vocab"),
        P(None, "vocab"),
        P(None, "vocab"),
    )
    out_specs = (P("batch", "vocab"),) * 5
    sizes = (mesh.shape["vocab"], mesh.shape["batch"])

    def whole(*args):
        return shards(sizes, *args)

    return jax.shard_map(whole, mesh=mesh, in_specs=in_specs, out_specs=out_specs, check_vma=False)
```

```python
import functools

import jax
import jax.numpy as jnp
from jax import lax
from jax.experimental import pallas as pl
from jax.experimental.pallas import tpu as pltpu
from jax.sharding import PartitionSpec as P


CLUSTERS = 4
CAP = 128
LANES = 128
SUBLANES = 8
F32 = jnp.float32
BF16 = jnp.bfloat16


VMEM = pl.BlockSpec(memory_space=pltpu.VMEM)
SMEM = pl.BlockSpec(memory_space=pltpu.SMEM)
HBM = pl.BlockSpec(memory_space=pltpu.HBM)


def matmul(left, right):
    return jnp.dot(left, right, preferred_element_type=F32)


def iota(shape, axis):
    return lax.broadcasted_iota(jnp.int32, shape, axis)


def placement(ids):
    count = ids.shape[1]
    onehot = (ids == iota((SUBLANES, count), 0)).astype(F32)
    earlier = (iota((count, count), 0) < iota((count, count), 1)).astype(BF16)
    before = matmul(onehot.astype(BF16), earlier)
    slot = jnp.sum(before * onehot, axis=0, keepdims=True)
    counts = jnp.sum(onehot, axis=1, keepdims=True)
    first, second = counts[0:1], counts[1:2]
    filler = before[2:3] + before[3:4] + first
    filler = jnp.where(filler < CAP, filler, filler + second)
    row = jnp.where(ids == 0, slot, jnp.where(ids == 1, slot + CAP, filler))
    return slot.astype(jnp.int32), row.astype(jnp.int32), counts


def row_matrix(row):
    count = row.shape[1]
    return (row == iota((count, count), 0)).astype(BF16)


def contract_last(left, right):
    return lax.dot_general(left, right, (((1,), (1,)), ((), ())), preferred_element_type=F32)


def partial_kernel(widths, spread, me_ref, mine_ref, ids_ref, columns_ref, proj_ref, *refs):
    outs, (ids, columns, proj, total, sems) = refs[:-5], refs[-5:]
    one, two = widths[0], widths[1]
    rest = widths[2] + widths[3]
    features = columns.shape[1]
    if columns_ref.shape[1] == features:
        source = columns_ref
    else:
        source = columns_ref.at[:, pl.ds(pl.multiple_of(me_ref[0] * features, LANES), features)]
    ranges = ((one + two, rest), (0, one), (one, two))
    copies = [pltpu.make_async_copy(source, columns, sems.at[0])]
    first_copy = pltpu.make_async_copy(ids_ref, ids, sems.at[4])
    first_copy.start()
    for at, (begin, size) in enumerate(ranges):
        copies.append(
            pltpu.make_async_copy(
                proj_ref.at[pl.ds(begin, size), :], proj.at[pl.ds(begin, size), :], sems.at[1 + at]
            )
        )
    for copy in copies:
        copy.start()
    first_copy.wait()
    _, row, counts = placement(ids[...])
    matrix = row_matrix(row)
    copies[0].wait()
    rows = matmul(matrix, columns[...]).astype(BF16)
    upper, lower = rows[:CAP], rows[CAP:]
    number = iota((CAP, 1), 0).astype(F32)
    copies[1].wait()
    others = contract_last(rows, proj[one + two :])
    copies[2].wait()
    whole = contract_last(upper, proj[:one])
    total[:, rest:one] = whole[:, rest:]
    total[:, :rest] = jnp.where(number < counts[0:1], whole[:, :rest], others[:CAP])
    copies[3].wait()
    whole = contract_last(lower, proj[one : one + two])
    total[:, one + rest :] = whole[:, rest:]
    total[:, one : one + rest] = jnp.where(number < counts[1:2], whole[:, :rest], others[CAP:])
    if spread:
        chunk = outs[0].shape[0]
        for step, out in enumerate(outs):
            begin = pl.multiple_of((me_ref[0] ^ step) * chunk, chunk)
            out[...] = total[pl.ds(begin, chunk), :]
    else:
        outs[0][...] = total[...]


def total_kernel(*refs):
    total = refs[0][...]
    for ref in refs[1:-1]:
        total = total + ref[...]
    refs[-1][...] = total.astype(BF16)


def unpack_kernel(ids_ref, pick_ref):
    ids = ids_ref[...]
    slot, row, _ = placement(ids)
    matrix = row_matrix(row)
    where = iota((CAP, ids.shape[1]), 0)
    for at, cluster in enumerate((2, 3)):
        own = ((ids == cluster) & (slot == where)).astype(BF16)
        pick_ref[at * CAP : (at + 1) * CAP, :] = contract_last(own, matrix).astype(BF16)


def pack_columns(columns):
    lane = iota((CAP, LANES), 1)
    square = jnp.zeros((CAP, LANES), F32)
    for at, column in enumerate(columns):
        square = jnp.where(lane == at, column, square)
    return square.T[:SUBLANES]


def row_stats(values):
    top = jnp.max(values, axis=1, keepdims=True)
    return top, jnp.sum(jnp.exp(values - top), axis=1, keepdims=True)


def head_more_kernel(steps, mine_ref, tokens_ref, *refs):
    weights, start, out = refs[:-2], refs[-2], refs[-1]
    total = start[...]
    for step, weight in zip(steps, weights):
        depth = weight.shape[0]
        begin = pl.multiple_of((mine_ref[0] ^ step) * depth, depth)
        total = total + matmul(tokens_ref[:, pl.ds(begin, depth)], weight[...])
    out[...] = total


def head_first_kernel(steps, mine_ref, tokens_ref, *refs):
    weights, out = refs[:-1], refs[-1]
    total = None
    for step, weight in zip(steps, weights):
        depth = weight.shape[0]
        begin = pl.multiple_of((mine_ref[0] ^ step) * depth, depth)
        part = matmul(tokens_ref[:, pl.ds(begin, depth)], weight[...])
        total = part if total is None else total + part
    out[...] = total


def head_last_kernel(steps, mine_ref, tokens_ref, *refs):
    weights, start, out, stats = refs[:-3], refs[-3], refs[-2], refs[-1]
    total = start[...]
    for step, weight in zip(steps, weights):
        depth = weight.shape[0]
        begin = pl.multiple_of((mine_ref[0] ^ step) * depth, depth)
        total = total + matmul(tokens_ref[:, pl.ds(begin, depth)], weight[...])
    out[...] = total
    top, mass = row_stats(total)
    stats[:SUBLANES] = pack_columns((top[:CAP], top[CAP:]))
    stats[SUBLANES:] = pack_columns((mass[:CAP], mass[CAP:]))


def score_kernel(widths, spread, me_ref, pick_ref, one_ref, two_ref, three_ref, four_ref, *refs):
    chunks = refs[:-6]
    scores, stats, joined = refs[-6:-2], refs[-2], refs[-1]
    if spread:
        chunk = chunks[0].shape[0]
        for step, ref in enumerate(chunks):
            begin = pl.multiple_of((me_ref[0] ^ step) * chunk, chunk)
            joined[pl.ds(begin, chunk), :] = ref[...]
    else:
        joined[...] = chunks[0][...]
    one, two = widths[0], widths[1]
    rest = widths[2] + widths[3]
    small = jnp.concatenate([joined[:, :rest], joined[:, one : one + rest]], axis=0)
    picked = matmul(pick_ref[...], small).astype(BF16)
    lefts = (
        joined[:, :one],
        joined[:, one : one + two],
        picked[:CAP, : widths[2]],
        picked[CAP:, widths[2] : rest],
    )
    tops, masses = [], []
    for left, weight, score in zip(lefts, (one_ref, two_ref, three_ref, four_ref), scores):
        value = matmul(left, weight[...])
        score[...] = value
        top, mass = row_stats(value)
        tops.append(top)
        masses.append(mass)
    zero = jnp.zeros((CAP, 1), F32)
    stats[:SUBLANES] = pack_columns([zero, zero] + tops)
    stats[SUBLANES:] = pack_columns([zero, zero] + masses)


def merge(own, other):
    top = jnp.maximum(own[:SUBLANES], other[:SUBLANES])
    mass = own[SUBLANES:] * jnp.exp(own[:SUBLANES] - top) + other[SUBLANES:] * jnp.exp(
        other[:SUBLANES] - top
    )
    return top, mass


def columns_of(rows):
    return jnp.concatenate([rows, jnp.zeros((LANES - SUBLANES, CAP), F32)], axis=0).T


def output_kernel(own_ref, other_ref, ids_ref, cluster_ref, head_ref, *refs):
    scores, head_out, outs = refs[:CLUSTERS], refs[CLUSTERS], refs[CLUSTERS + 1 :]
    ids = ids_ref[...]
    slot, _, counts = placement(ids)
    cluster_logits = cluster_ref[...]
    own_logit = jnp.sum(
        jnp.where(ids == iota(cluster_logits.shape, 0), cluster_logits, 0.0), axis=0, keepdims=True
    )
    top, mass = merge(own_ref[...], other_ref[...])
    head_top = jnp.concatenate([top[0:1], top[1:2]], axis=1)
    head_mass = jnp.concatenate([mass[0:1], mass[1:2]], axis=1)
    overall = jnp.maximum(head_top, jnp.max(cluster_logits, axis=0, keepdims=True))
    denominator = head_mass * jnp.exp(head_top - overall) + jnp.sum(
        jnp.exp(cluster_logits - overall), axis=0, keepdims=True
    )
    log_total = overall + jnp.log(denominator)
    number = iota((SUBLANES, CAP), 0)
    logs = jnp.where(
        number == 0, log_total[:, :CAP], jnp.where(number == 1, log_total[:, CAP:], top + jnp.log(mass))
    )
    columns = columns_of(logs)
    head_out[:CAP] = head_ref[:CAP] - columns[:, 0:1]
    head_out[CAP:] = head_ref[CAP:] - columns[:, 1:2]
    own_logp = own_logit - log_total
    here = slot == iota((CAP, ids.shape[1]), 0)
    number = iota((CAP, 1), 0).astype(F32)
    for cluster in range(CLUSTERS):
        slot_logp = jnp.sum(jnp.where((ids == cluster) & here, own_logp, 0.0), axis=1, keepdims=True)
        shift = columns[:, 2 + cluster : 3 + cluster] - slot_logp
        outs[cluster][...] = jnp.where(
            number < counts[cluster : cluster + 1], scores[cluster][...] - shift, 0.0
        )


def shapes(*pairs):
    return [jax.ShapeDtypeStruct(shape, kind) for shape, kind in pairs]


def in_hbm(value):
    return pltpu.with_memory_space_constraint(value, pltpu.HBM)


def in_vmem(value):
    return pltpu.with_memory_space_constraint(value, pltpu.VMEM)


def limit(mebibytes):
    return pltpu.CompilerParams(vmem_limit_bytes=mebibytes * 2**20)


def cost(flops, size):
    return pl.CostEstimate(flops=int(flops), bytes_accessed=int(size), transcendentals=0)


def shards(
    sizes,
    tokens,
    cluster_ids,
    head_weight,
    cluster_weight,
    tail_proj,
    out_one,
    out_two,
    out_three,
    out_four,
):
    members, groups = sizes
    me = lax.axis_index("vocab")
    mine = lax.axis_index("batch")
    out_weights = (out_one, out_two, out_three, out_four)
    widths = tuple(weight.shape[0] for weight in out_weights)
    packed = widths[0] + widths[1]
    chunk = CAP // members
    spread = chunk % 16 == 0
    count = tokens.shape[0]

    def exchange(value, axis, size, step):
        return lax.ppermute(value, axis, [(at, at ^ step) for at in range(size)])

    features = tail_proj.shape[0]
    ids = cluster_ids.T
    if features % LANES:
        columns = lax.dynamic_slice_in_dim(tokens, me * features, features, 1)
    else:
        columns = tokens
    me_index = me.reshape(1).astype(jnp.int32)
    mine_index = mine.reshape(1).astype(jnp.int32)
    parts = pl.pallas_call(
        functools.partial(partial_kernel, widths, spread),
        out_shape=shapes(*([((chunk, packed), F32)] * members if spread else [((CAP, packed), F32)])),
        in_specs=[SMEM, SMEM, HBM, HBM, HBM],
        out_specs=[VMEM] * (members if spread else 1),
        scratch_shapes=[
            pltpu.VMEM((1, count), jnp.int32),
            pltpu.VMEM((count, features), BF16),
            pltpu.VMEM(tail_proj.shape[::-1], BF16),
            pltpu.VMEM((CAP, packed), F32),
            pltpu.SemaphoreType.DMA((5,)),
        ],
        compiler_params=limit(8),
        cost_estimate=cost(2 * count * features * 2 * packed, 4 * features * packed),
        name="partial",
    )(me_index, mine_index, in_hbm(ids), in_hbm(columns), in_hbm(tail_proj.T))
    if not spread:
        parts = [
            lax.dynamic_slice_in_dim(parts[0], (me ^ step) * chunk, chunk, 0) for step in range(members)
        ]
    parts, head_weight = lax.optimization_barrier((parts, head_weight))
    pairs = [
        parts[step] + exchange(parts[step + 1], "vocab", members, 1)
        for step in reversed(range(0, members, 2))
    ][::-1]
    arrived = [pairs[0]] + [exchange(pairs[at], "vocab", members, 2 * at) for at in reversed(range(1, members // 2))]

    steps = [step for step in range(0, groups, 2)]
    far = [exchange(head_weight, "batch", groups, step) for step in steps[1:]]
    near = exchange(head_weight, "batch", groups, 1)
    vocab = head_weight.shape[1]
    depth = head_weight.shape[0]
    head_start = pl.pallas_call(
        functools.partial(head_first_kernel, (0, 1)),
        out_shape=shapes(((count, vocab), F32))[0],
        in_specs=[SMEM, VMEM, VMEM, VMEM],
        out_specs=VMEM,
        compiler_params=limit(6),
        cost_estimate=cost(2 * count * vocab * depth * 2, depth * vocab * 4),
        name="head_first",
    )(mine_index, tokens, head_weight, near)
    pick = pl.pallas_call(
        unpack_kernel,
        out_shape=shapes(((2 * CAP, count), BF16))[0],
        in_specs=[VMEM],
        out_specs=VMEM,
        compiler_params=limit(2),
        cost_estimate=cost(2 * count * count * count * 2, 4 * count * count),
        name="unpack",
    )(ids)
    cluster_logits = lax.dot_general(
        cluster_weight, tokens, (((0,), (1,)), ((), ())), preferred_element_type=F32
    )
    arrived, head_start, cluster_logits = lax.optimization_barrier((arrived, head_start, cluster_logits))
    own = pl.pallas_call(
        total_kernel,
        out_shape=shapes(((chunk, packed), BF16))[0],
        in_specs=[VMEM] * len(arrived),
        out_specs=VMEM,
        compiler_params=limit(2),
        cost_estimate=cost(chunk * packed * len(arrived), 4 * chunk * packed * len(arrived)),
        name="total",
    )(*map(in_vmem, arrived))
    evens = [own] + [exchange(own, "vocab", members, step) for step in range(2, members, 2)]
    _, far = lax.optimization_barrier((evens[-1], far))
    chunks = []
    for value in evens:
        chunks += [value, exchange(value, "vocab", members, 1)]
    if not spread:
        stacked = jnp.stack(chunks)
        order = me ^ jnp.arange(members)
        chunks = [jnp.take(stacked, order, axis=0).reshape(CAP, packed)]

    rest = [exchange(value, "batch", groups, 1) for value in far]
    head_more = pl.pallas_call(
        functools.partial(head_more_kernel, tuple(steps[1:])),
        out_shape=shapes(((count, vocab), F32))[0],
        in_specs=[SMEM] + [VMEM] * (len(far) + 2),
        out_specs=VMEM,
        compiler_params=limit(6),
        cost_estimate=cost(2 * count * vocab * depth * len(far), depth * vocab * 4),
        name="head_more",
    )(mine_index, tokens, *map(in_vmem, far), head_start)
    head_logits, head_stats = pl.pallas_call(
        functools.partial(head_last_kernel, tuple(step ^ 1 for step in steps[1:])),
        out_shape=shapes(((count, vocab), F32), ((2 * SUBLANES, CAP), F32)),
        in_specs=[SMEM] + [VMEM] * (len(rest) + 2),
        out_specs=[VMEM] * 2,
        compiler_params=limit(6),
        cost_estimate=cost(2 * count * vocab * depth * len(rest), depth * vocab * 4),
        name="head_last",
    )(mine_index, tokens, *rest, head_more)
    score_shapes = [((CAP, weight.shape[1]), F32) for weight in out_weights]
    *scores, stats = pl.pallas_call(
        functools.partial(score_kernel, widths, spread),
        out_shape=shapes(*score_shapes, ((2 * SUBLANES, CAP), F32)),
        in_specs=[SMEM] + [VMEM] * (5 + len(chunks)),
        out_specs=[VMEM] * (CLUSTERS + 1),
        scratch_shapes=[pltpu.VMEM((CAP, packed), BF16)],
        compiler_params=limit(6),
        cost_estimate=cost(
            2 * CAP * sum(weight.size for weight in out_weights), 2 * sum(weight.size for weight in out_weights)
        ),
        name="scores",
    )(me_index, pick, *out_weights, *chunks)

    stats = jnp.where(lax.rem(iota(stats.shape, 0), SUBLANES) < 2, head_stats, stats)
    step = 1
    while 2 * step < members:
        stats = jnp.concatenate(merge(stats, exchange(stats, "vocab", members, step)), axis=0)
        step = 2 * step
    other = exchange(stats, "vocab", members, step)
    out_shapes = [((count, vocab), F32)] + score_shapes
    return tuple(
        pl.pallas_call(
            output_kernel,
            out_shape=shapes(*out_shapes),
            in_specs=[VMEM] * (5 + CLUSTERS),
            out_specs=[VMEM] * (1 + CLUSTERS),
            compiler_params=limit(6),
        cost_estimate=cost(count * vocab * 8, 8 * count * vocab * 8),
            name="outputs",
        )(stats, other, ids, cluster_logits, head_logits, *scores)
    )


def solution(mesh):
    in_specs = (
        P("batch", None),
        P("batch", None),
        P("batch", "vocab"),
        P(),
        P("vocab", None),
        P(None, "vocab"),
        P(None, "vocab"),
        P(None, "vocab"),
        P(None, "vocab"),
    )
    out_specs = (P("batch", "vocab"),) * 5
    sizes = (mesh.shape["vocab"], mesh.shape["batch"])

    def whole(*args):
        return shards(sizes, *args)

    return jax.shard_map(whole, mesh=mesh, in_specs=in_specs, out_specs=out_specs, check_vma=False)
```

```python
import functools

import jax
import jax.numpy as jnp
from jax import lax
from jax.experimental import pallas as pl
from jax.experimental.pallas import tpu as pltpu
from jax.sharding import PartitionSpec as P


CLUSTERS = 4
CAP = 128
LANES = 128
SUBLANES = 8
F32 = jnp.float32
BF16 = jnp.bfloat16


VMEM = pl.BlockSpec(memory_space=pltpu.VMEM)
SMEM = pl.BlockSpec(memory_space=pltpu.SMEM)
HBM = pl.BlockSpec(memory_space=pltpu.HBM)


def matmul(left, right):
    return jnp.dot(left, right, preferred_element_type=F32)


def iota(shape, axis):
    return lax.broadcasted_iota(jnp.int32, shape, axis)


def placement(ids):
    count = ids.shape[1]
    onehot = (ids == iota((SUBLANES, count), 0)).astype(F32)
    earlier = (iota((count, count), 0) < iota((count, count), 1)).astype(BF16)
    before = matmul(onehot.astype(BF16), earlier)
    slot = jnp.sum(before * onehot, axis=0, keepdims=True)
    counts = jnp.sum(onehot, axis=1, keepdims=True)
    first, second = counts[0:1], counts[1:2]
    filler = before[2:3] + before[3:4] + first
    filler = jnp.where(filler < CAP, filler, filler + second)
    row = jnp.where(ids == 0, slot, jnp.where(ids == 1, slot + CAP, filler))
    return slot.astype(jnp.int32), row.astype(jnp.int32), counts


def row_matrix(row):
    count = row.shape[1]
    return (row == iota((count, count), 0)).astype(BF16)


def contract_last(left, right):
    return lax.dot_general(left, right, (((1,), (1,)), ((), ())), preferred_element_type=F32)


def partial_kernel(widths, spread, me_ref, mine_ref, ids_ref, columns_ref, proj_ref, head_ref, *refs):
    outs, cuts, (ids, columns, proj, total, sems) = refs[:-7], refs[-7:-5], refs[-5:]
    one, two = widths[0], widths[1]
    rest = widths[2] + widths[3]
    features = columns.shape[1]
    if columns_ref.shape[1] == features:
        source = columns_ref
    else:
        source = columns_ref.at[:, pl.ds(pl.multiple_of(me_ref[0] * features, LANES), features)]
    ranges = ((one + two, rest), (0, one), (one, two))
    copies = [pltpu.make_async_copy(source, columns, sems.at[0])]
    first_copy = pltpu.make_async_copy(ids_ref, ids, sems.at[4])
    first_copy.start()
    for at, (begin, size) in enumerate(ranges):
        copies.append(
            pltpu.make_async_copy(
                proj_ref.at[pl.ds(begin, size), :], proj.at[pl.ds(begin, size), :], sems.at[1 + at]
            )
        )
    begin = 0
    for at, cut in enumerate(cuts):
        copies.append(pltpu.make_async_copy(head_ref.at[pl.ds(begin, cut.shape[0]), :], cut, sems.at[5 + at]))
        begin += cut.shape[0]
    for copy in copies:
        copy.start()
    first_copy.wait()
    _, row, counts = placement(ids[...])
    matrix = row_matrix(row)
    copies[0].wait()
    rows = matmul(matrix, columns[...]).astype(BF16)
    upper, lower = rows[:CAP], rows[CAP:]
    number = iota((CAP, 1), 0).astype(F32)
    copies[1].wait()
    others = contract_last(rows, proj[one + two :])
    copies[2].wait()
    whole = contract_last(upper, proj[:one])
    total[:, rest:one] = whole[:, rest:]
    total[:, :rest] = jnp.where(number < counts[0:1], whole[:, :rest], others[:CAP])
    copies[3].wait()
    whole = contract_last(lower, proj[one : one + two])
    total[:, one + rest :] = whole[:, rest:]
    total[:, one : one + rest] = jnp.where(number < counts[1:2], whole[:, :rest], others[CAP:])
    if spread:
        chunk = outs[0].shape[0]
        step = 0
        for out in outs:
            for first in range(0, out.shape[0], chunk):
                begin = pl.multiple_of((me_ref[0] ^ step) * chunk, chunk)
                out[first : first + chunk, :] = total[pl.ds(begin, chunk), :]
                step += 1
    else:
        outs[0][...] = total[...]
    for copy in copies[4:]:
        copy.wait()


def total_kernel(*refs):
    total = refs[0][: refs[-1].shape[0]]
    for ref in refs[1:-1]:
        total = total + ref[...]
    refs[-1][...] = total.astype(BF16)


def unpack_kernel(cluster, ids_ref, pick_ref):
    ids = ids_ref[...]
    slot, row, _ = placement(ids)
    own = ((ids == cluster) & (slot == iota((CAP, ids.shape[1]), 0))).astype(BF16)
    pick_ref[...] = contract_last(own, row_matrix(row)).astype(BF16)


def pack_columns(columns):
    lane = iota((CAP, LANES), 1)
    square = jnp.zeros((CAP, LANES), F32)
    for at, column in enumerate(columns):
        square = jnp.where(lane == at, column, square)
    return square.T[:SUBLANES]


def row_stats(values):
    top = jnp.max(values, axis=1, keepdims=True)
    return top, jnp.sum(jnp.exp(values - top), axis=1, keepdims=True)


def add_pieces(total, places, mine_ref, tokens_ref, weights):
    for (step, depth, first), weight in zip(places, weights):
        begin = pl.multiple_of((mine_ref[0] ^ step) * depth + first, LANES)
        total = total + matmul(tokens_ref[:, pl.ds(begin, weight.shape[0])], weight[...])
    return total


def head_more_kernel(places, mine_ref, tokens_ref, *refs):
    weights, start, out = refs[:-2], refs[-2], refs[-1]
    out[...] = add_pieces(start[...], places, mine_ref, tokens_ref, weights)


def head_first_kernel(steps, mine_ref, tokens_ref, *refs):
    count = len(steps)
    weights, sources, out, kept, sems = (
        refs[:count],
        refs[count : count + CLUSTERS],
        refs[count + CLUSTERS],
        refs[count + CLUSTERS + 1 : -1],
        refs[-1],
    )
    copies = [
        pltpu.make_async_copy(source, value, sems.at[at]) for at, (source, value) in enumerate(zip(sources, kept))
    ]
    for copy in copies:
        copy.start()
    total = None
    for step, weight in zip(steps, weights):
        depth = weight.shape[0]
        begin = pl.multiple_of((mine_ref[0] ^ step) * depth, depth)
        part = matmul(tokens_ref[:, pl.ds(begin, depth)], weight[...])
        total = part if total is None else total + part
    out[...] = total
    for copy in copies:
        copy.wait()


def head_last_kernel(places, mine_ref, tokens_ref, *refs):
    weights, start, out, stats = refs[:-3], refs[-3], refs[-2], refs[-1]
    total = add_pieces(start[...], places, mine_ref, tokens_ref, weights)
    out[...] = total
    top, mass = row_stats(total)
    stats[:SUBLANES] = pack_columns((top[:CAP], top[CAP:]))
    stats[SUBLANES:] = pack_columns((mass[:CAP], mass[CAP:]))


def score_kernel(widths, spread, me_ref, three_pick_ref, four_pick_ref, one_ref, two_ref, three_ref, four_ref, *refs):
    chunks = refs[:-6]
    scores, stats, joined = refs[-6:-2], refs[-2], refs[-1]
    if spread:
        chunk = chunks[0].shape[0]
        for step, ref in enumerate(chunks):
            begin = pl.multiple_of((me_ref[0] ^ step) * chunk, chunk)
            joined[pl.ds(begin, chunk), :] = ref[...]
    else:
        joined[...] = chunks[0][...]
    one, two = widths[0], widths[1]
    rest = widths[2] + widths[3]
    small = jnp.concatenate([joined[:, :rest], joined[:, one : one + rest]], axis=0)
    lefts = (
        joined[:, :one],
        joined[:, one : one + two],
        matmul(three_pick_ref[...], small[:, : widths[2]]).astype(BF16),
        matmul(four_pick_ref[...], small[:, widths[2] :]).astype(BF16),
    )
    tops, masses = [], []
    for left, weight, score in zip(lefts, (one_ref, two_ref, three_ref, four_ref), scores):
        value = matmul(left, weight[...])
        score[...] = value
        top, mass = row_stats(value)
        tops.append(top)
        masses.append(mass)
    zero = jnp.zeros((CAP, 1), F32)
    stats[:SUBLANES] = pack_columns([zero, zero] + tops)
    stats[SUBLANES:] = pack_columns([zero, zero] + masses)


def merge(own, other):
    top = jnp.maximum(own[:SUBLANES], other[:SUBLANES])
    mass = own[SUBLANES:] * jnp.exp(own[:SUBLANES] - top) + other[SUBLANES:] * jnp.exp(
        other[:SUBLANES] - top
    )
    return top, mass


def columns_of(rows):
    return jnp.concatenate([rows, jnp.zeros((LANES - SUBLANES, CAP), F32)], axis=0).T


def output_kernel(own_ref, other_ref, ids_ref, cluster_ref, head_ref, *refs):
    scores, targets, values, sems = refs[:CLUSTERS], refs[CLUSTERS:9], refs[9:14], refs[14]
    copies = [
        pltpu.make_async_copy(value, target, sems.at[at])
        for at, (value, target) in enumerate(zip(values, targets))
    ]
    head_out, outs = values[0], values[1:]
    ids = ids_ref[...]
    slot, _, counts = placement(ids)
    cluster_logits = cluster_ref[...]
    own_logit = jnp.sum(
        jnp.where(ids == iota(cluster_logits.shape, 0), cluster_logits, 0.0), axis=0, keepdims=True
    )
    top, mass = merge(own_ref[...], other_ref[...])
    head_top = jnp.concatenate([top[0:1], top[1:2]], axis=1)
    head_mass = jnp.concatenate([mass[0:1], mass[1:2]], axis=1)
    overall = jnp.maximum(head_top, jnp.max(cluster_logits, axis=0, keepdims=True))
    denominator = head_mass * jnp.exp(head_top - overall) + jnp.sum(
        jnp.exp(cluster_logits - overall), axis=0, keepdims=True
    )
    log_total = overall + jnp.log(denominator)
    number = iota((SUBLANES, CAP), 0)
    logs = jnp.where(
        number == 0, log_total[:, :CAP], jnp.where(number == 1, log_total[:, CAP:], top + jnp.log(mass))
    )
    columns = columns_of(logs)
    head_out[:CAP] = head_ref[:CAP] - columns[:, 0:1]
    head_out[CAP:] = head_ref[CAP:] - columns[:, 1:2]
    copies[0].start()
    own_logp = own_logit - log_total
    here = slot == iota((CAP, ids.shape[1]), 0)
    number = iota((CAP, 1), 0).astype(F32)
    for cluster in range(CLUSTERS):
        slot_logp = jnp.sum(jnp.where((ids == cluster) & here, own_logp, 0.0), axis=1, keepdims=True)
        shift = columns[:, 2 + cluster : 3 + cluster] - slot_logp
        outs[cluster][...] = jnp.where(
            number < counts[cluster : cluster + 1], scores[cluster][...] - shift, 0.0
        )
        copies[1 + cluster].start()
    for copy in copies:
        copy.wait()


def shapes(*pairs):
    return [jax.ShapeDtypeStruct(shape, kind) for shape, kind in pairs]


def in_hbm(value):
    return pltpu.with_memory_space_constraint(value, pltpu.HBM)


def in_vmem(value):
    return pltpu.with_memory_space_constraint(value, pltpu.VMEM)


def limit(mebibytes):
    return pltpu.CompilerParams(vmem_limit_bytes=mebibytes * 2**20)


def cost(flops, size):
    return pl.CostEstimate(flops=int(flops), bytes_accessed=int(size), transcendentals=0)


def shards(
    sizes,
    tokens,
    cluster_ids,
    head_weight,
    cluster_weight,
    tail_proj,
    out_one,
    out_two,
    out_three,
    out_four,
):
    members, groups = sizes
    me = lax.axis_index("vocab")
    mine = lax.axis_index("batch")
    out_weights = (out_one, out_two, out_three, out_four)
    widths = tuple(weight.shape[0] for weight in out_weights)
    packed = widths[0] + widths[1]
    chunk = CAP // members
    spread = chunk % 16 == 0
    count = tokens.shape[0]

    def exchange(value, axis, size, step):
        return lax.ppermute(value, axis, [(at, at ^ step) for at in range(size)])

    features = tail_proj.shape[0]
    ids = cluster_ids.T
    if features % LANES:
        columns = lax.dynamic_slice_in_dim(tokens, me * features, features, 1)
    else:
        columns = tokens
    heights = [chunk, chunk, 2 * chunk] + [chunk] * (members - 4) if spread else [CAP]
    me_index = me.reshape(1).astype(jnp.int32)
    mine_index = mine.reshape(1).astype(jnp.int32)
    depth, vocab = head_weight.shape
    large = depth * 3 // 4 // LANES * LANES
    *parts, cut_one, cut_two = pl.pallas_call(
        functools.partial(partial_kernel, widths, spread),
        out_shape=[pltpu.VMEM((rows, packed), F32) for rows in heights]
        + [pltpu.VMEM((rows, vocab), BF16) for rows in (large, depth - large)],
        in_specs=[SMEM, SMEM, HBM, HBM, HBM, HBM],
        out_specs=[VMEM] * (len(heights) + 2),
        scratch_shapes=[
            pltpu.VMEM((1, count), jnp.int32),
            pltpu.VMEM((count, features), BF16),
            pltpu.VMEM(tail_proj.shape[::-1], BF16),
            pltpu.VMEM((CAP, packed), F32),
            pltpu.SemaphoreType.DMA((7,)),
        ],
        compiler_params=limit(8),
        cost_estimate=cost(2 * count * features * 2 * packed, 4 * features * packed),
        name="partial",
    )(me_index, mine_index, in_hbm(ids), in_hbm(columns), in_hbm(tail_proj.T), in_hbm(head_weight))
    if not spread:
        blocks = [
            lax.dynamic_slice_in_dim(parts[0], (me ^ step) * chunk, chunk, 0) for step in range(members)
        ]
        parts = blocks[:2] + [jnp.concatenate(blocks[2:4], axis=0)] + blocks[4:]
    parts, head_weight = lax.optimization_barrier((parts, head_weight))
    cuts = (cut_one, cut_two)
    beside = exchange(parts[2], "vocab", members, 2)
    last = exchange(parts[1] + beside[chunk:], "vocab", members, 1)
    arrived = [beside, parts[0], last]
    for step in range(members - 2, 2, -2):
        pair = parts[step - 1] + exchange(parts[step], "vocab", members, 1)
        arrived.append(exchange(pair, "vocab", members, step))

    steps = [step for step in range(0, groups, 2)]
    far = [[exchange(cut, "batch", groups, step) for step in steps[1:]] for cut in cuts]
    near = exchange(head_weight, "batch", groups, 1)
    head_start, *out_weights = pl.pallas_call(
        functools.partial(head_first_kernel, (0, 1)),
        out_shape=[pltpu.VMEM((count, vocab), F32)]
        + [pltpu.VMEM(weight.shape, weight.dtype) for weight in out_weights],
        in_specs=[SMEM, VMEM, VMEM, VMEM] + [HBM] * CLUSTERS,
        out_specs=[VMEM] * (1 + CLUSTERS),
        scratch_shapes=[pltpu.SemaphoreType.DMA((CLUSTERS,))],
        compiler_params=limit(6),
        cost_estimate=cost(2 * count * vocab * depth * 2, depth * vocab * 4),
        name="head_first",
    )(mine_index, tokens, head_weight, near, *map(in_hbm, out_weights))
    picks = [
        pl.pallas_call(
            functools.partial(unpack_kernel, cluster),
            out_shape=pltpu.VMEM((CAP, count), BF16),
            in_specs=[VMEM],
            out_specs=VMEM,
            compiler_params=limit(2),
            cost_estimate=cost(2 * count * count * count, 4 * count * count),
        )(ids)
        for cluster in (2, 3)
    ]
    cluster_logits = lax.dot_general(
        cluster_weight, tokens, (((0,), (1,)), ((), ())), preferred_element_type=F32
    )
    arrived, head_start, cluster_logits = lax.optimization_barrier((arrived, head_start, cluster_logits))
    own = pl.pallas_call(
        total_kernel,
        out_shape=shapes(((chunk, packed), BF16))[0],
        in_specs=[VMEM] * len(arrived),
        out_specs=VMEM,
        compiler_params=limit(2),
        cost_estimate=cost(chunk * packed * len(arrived), 4 * chunk * packed * len(arrived)),
        name="total",
    )(*map(in_vmem, arrived))
    evens = [own] + [exchange(own, "vocab", members, step) for step in range(2, members, 2)]
    _, far[1] = lax.optimization_barrier((evens[-1], far[1]))
    _, far[0] = lax.optimization_barrier((own, far[0]))
    chunks = []
    for value in evens:
        chunks += [value, exchange(value, "vocab", members, 1)]
    if not spread:
        stacked = jnp.stack(chunks)
        order = me ^ jnp.arange(members)
        chunks = [jnp.take(stacked, order, axis=0).reshape(CAP, packed)]

    rest = [[exchange(value, "batch", groups, 1) for value in values] for values in far]
    early = far[0] + rest[0] + far[1]
    places = [
        [(step ^ near, depth, first) for step in steps[1:]]
        for first, near in ((0, 0), (0, 1), (large, 0), (large, 1))
    ]
    head_more = pl.pallas_call(
        functools.partial(head_more_kernel, sum(places[:3], [])),
        out_shape=shapes(((count, vocab), F32))[0],
        in_specs=[SMEM] + [VMEM] * (len(early) + 2),
        out_specs=VMEM,
        compiler_params=limit(6),
        cost_estimate=cost(2 * count * vocab * depth * 2, depth * vocab * 4),
        name="head_more",
    )(mine_index, tokens, *map(in_vmem, early), head_start)
    head_logits, head_stats = pl.pallas_call(
        functools.partial(head_last_kernel, places[3]),
        out_shape=shapes(((count, vocab), F32), ((2 * SUBLANES, CAP), F32)),
        in_specs=[SMEM] + [VMEM] * (len(rest[1]) + 2),
        out_specs=[VMEM] * 2,
        compiler_params=limit(6),
        cost_estimate=cost(2 * count * vocab * depth * len(rest[1]), depth * vocab * 4),
        name="head_last",
    )(mine_index, tokens, *rest[1], head_more)
    score_shapes = [((CAP, weight.shape[1]), F32) for weight in out_weights]
    *scores, stats = pl.pallas_call(
        functools.partial(score_kernel, widths, spread),
        out_shape=shapes(*score_shapes, ((2 * SUBLANES, CAP), F32)),
        in_specs=[SMEM] + [VMEM] * (6 + len(chunks)),
        out_specs=[VMEM] * (CLUSTERS + 1),
        scratch_shapes=[pltpu.VMEM((CAP, packed), BF16)],
        compiler_params=limit(6),
        cost_estimate=cost(
            2 * CAP * sum(weight.size for weight in out_weights), 2 * sum(weight.size for weight in out_weights)
        ),
        name="scores",
    )(me_index, *picks, *out_weights, *chunks)

    stats = jnp.where(lax.rem(iota(stats.shape, 0), SUBLANES) < 2, head_stats, stats)
    step = members // 2
    while step > 1:
        stats = jnp.concatenate(merge(stats, exchange(stats, "vocab", members, step)), axis=0)
        step = step // 2
    other = exchange(stats, "vocab", members, 1)
    out_shapes = [((count, vocab), F32)] + score_shapes
    return tuple(
        pl.pallas_call(
            output_kernel,
            out_shape=shapes(*out_shapes),
            in_specs=[VMEM] * (5 + CLUSTERS),
            out_specs=[HBM] * (1 + CLUSTERS),
            scratch_shapes=[pltpu.VMEM(shape, kind) for shape, kind in out_shapes]
            + [pltpu.SemaphoreType.DMA((1 + CLUSTERS,))],
            compiler_params=limit(6),
        cost_estimate=cost(count * vocab * 8, 8 * count * vocab * 8),
            name="outputs",
        )(stats, other, ids, cluster_logits, head_logits, *scores)
    )


def solution(mesh):
    in_specs = (
        P("batch", None),
        P("batch", None),
        P("batch", "vocab"),
        P(),
        P("vocab", None),
        P(None, "vocab"),
        P(None, "vocab"),
        P(None, "vocab"),
        P(None, "vocab"),
    )
    out_specs = (P("batch", "vocab"),) * 5
    sizes = (mesh.shape["vocab"], mesh.shape["batch"])

    def whole(*args):
        return shards(sizes, *args)

    return jax.shard_map(whole, mesh=mesh, in_specs=in_specs, out_specs=out_specs, check_vma=False)
```
